32 devices in a mesh: gx: 4 (over x, core), gy: 4 (over z), gz: 2 (over y).
Axes of the slice: x: 2, y: 2, z: 4, core: 2. Of those that a mesh axis runs over, the one named last changes fastest.
Arguments:
- layer_input: bfloat16 [1024, 4096], P('gz', ('gx', 'gy')), may hold values from -6 to 6
- modality: int32 [1024], P('gz'), may hold values 0 or 1
- image_spans: int32 [2, 8], replicated, may hold values from 0 to 1024, as said below
- norm_gain: float32 [2, 4096], P(None, ('gx', 'gy')), may hold values from 0.1 to 1.9
- w_qkv: bfloat16 [3, 4096, 2048], P(None, 'gz', ('gx', 'gy')), as said below
- w_out: bfloat16 [2048, 4096], P(('gx', 'gy'), 'gz'), may hold values from -0.125 to 0.125
- grad_out: bfloat16 [1024, 4096], P('gz', ('gx', 'gy')), may hold values from -6 to 6
Outputs:
- attn_out: bfloat16 [1024, 4096], P('gz', ('gx', 'gy'))
- grad_in: bfloat16 [1024, 4096], P('gz', ('gx', 'gy'))
- grad_qkv: float32 [3, 4096, 2048], P(None, 'gz', ('gx', 'gy'))
- grad_wout: float32 [2048, 4096], P(('gx', 'gy'), 'gz')
- grad_gain: float32 [2, 4096], P(None, ('gx', 'gy'))
The draws below stay inside these ranges and needn't reach their ends.
Inputs may be any that keep to these rules, and one draw needn't show every extreme that they name: `image_spans`: row 0 holds the first position of each of 8 image spans, in increasing order, and row 1 one past its last; spans are disjoint and none is empty. `w_qkv`: entries are at most 20 * 4096 ** -0.5 in magnitude.
All inputs are finite; a program needn't handle non-finite values. No bound on the sum of `modality` on one device may be relied on, other than what follows from the above.
Results may differ from the reference program's by a relative error of at most 0.035.
The reference program's roundings to bfloat16 on the way (of `normed`, `queries`, `attended`, `d_attended`, `d_scores`, `d_queries` and `d_keys`) count: a program that leaves them out, or rounds other values in their place, can miss the bound.
Values may be sent and summed in bfloat16 or wider, within the bound.
A program may use at most 128 MiB of HBM per device.

```python
import math
import jax
import jax.numpy as jnp
from jax import lax

D = 4096
HEAD_DIM = 128
TOK_DEV = 512
SPANS = 8
HEADS = 16
TOKENS = 1024
N_GX = 4
N_GY = 4
N_GZ = 2


def draw_image_spans(key, part):
    stride = TOKENS // SPANS
    key_one, key_two = jax.random.split(jax.random.fold_in(key, 11))
    labels = jnp.arange(SPANS, dtype=jnp.int32)
    offset = jax.random.randint(key_one, (SPANS,), 0, max(stride // 4, 1))
    length = jax.random.randint(key_two, (SPANS,), max(stride // 4, 1), stride // 2 + 1)
    starts = labels * stride + stride // 2 + offset
    finish = jnp.minimum(starts + length, TOKENS)
    return jnp.stack([starts, finish]).astype(jnp.int32)


def draw_w_qkv(key, part):
    key_one = jax.random.fold_in(jax.random.fold_in(key, 23), 0)
    weights = jax.random.truncated_normal(key_one, -4.0, 4.0, (3, D, HEADS * HEAD_DIM), jnp.float32) * D ** (-0.5)
    return weights.astype(jnp.bfloat16)


def with_ends(entries, stream_key, least, top_value):
    longest = entries.shape.index(max(entries.shape))
    spots = []
    for shift in (0, 1):
        where = [jax.random.randint(jax.random.fold_in(stream_key, axis), (), 0, length) for axis, length in enumerate(entries.shape)]
        where[longest] = (where[longest] + shift) % entries.shape[longest]
        spots.append(tuple(where))
    return entries.at[spots[0]].set(least).at[spots[1]].set(top_value)


def level_of(rng, dims, cuts, smallest, high):
    loudness = 1.0
    for position, blocks in cuts:
        steps = jax.random.uniform(jax.random.fold_in(jax.random.fold_in(rng, 6), position), (blocks,), jnp.float32, smallest / len(cuts), high / len(cuts))
        loudness = loudness * jnp.repeat(jnp.exp(steps), dims[position] // blocks).reshape((-1,) + (1,) * (len(dims) - 1 - position))
    return loudness


def scatter_about(own_key, shape, deviation, bound, cuts=(), kind=jnp.bfloat16):
    drawn = jax.random.normal(own_key, shape, jnp.float32) * deviation
    if len(cuts) > 0:
        drawn = level_of(own_key, shape, cuts, -0.22, 0.18) * drawn
    return jnp.clip(drawn, min=-bound, max=bound).astype(kind)


def setup_inputs(seed: int = 0) -> dict:
    splits = jax.random.split(jax.random.key(seed), 8)
    return {
        "layer_input": scatter_about(splits[0], (TOKENS, D), 1.0, 6.0, ((0, 2), (1, 16))),
        "modality": with_ends((jax.random.randint(splits[1], (TOKENS,), 0, 2) < 1).astype(jnp.int32), jax.random.fold_in(splits[1], 1), 0, 1),
        "image_spans": draw_image_spans(jax.random.fold_in(splits[7], 71), 0),
        "norm_gain": jnp.clip(1.0 + 0.18 * jax.random.normal(splits[3], (2, D), jnp.float32), 0.1, 1.9),
        "w_qkv": draw_w_qkv(jax.random.fold_in(splits[7], 71), 0),
        "w_out": scatter_about(splits[5], (HEADS * HEAD_DIM, D), (HEADS * HEAD_DIM) ** -0.5, 0.125, ((0, 16), (1, 2))),
        "grad_out": scatter_about(splits[6], (TOKENS, D), 1.0, 6.0, ((0, 2), (1, 16))),
    }


epsilon = 1e-05
masked_low = -1e+30

def span_index(positions, image_spans):
    inside = (positions[:, None] >= image_spans[0][None, :]) & (positions[:, None] < image_spans[1][None, :])
    labels = jnp.arange(1, image_spans.shape[1] + 1, dtype=jnp.int32)
    return (lax.optimization_barrier(jnp.sum(jnp.where(inside, labels[None, :], 0), axis=1)) - 1).astype(jnp.int32)

def visible(query_pos, query_span, key_pos, key_span):
    causal = key_pos[None, :] <= query_pos[:, None]
    same_image = (query_span[:, None] == key_span[None, :]) & (query_span[:, None] >= 0)
    return causal | same_image

def rounded(value):
    return lax.optimization_barrier(value.astype(jnp.bfloat16)).astype(jnp.float32)

def reference(layer_input, modality, image_spans, norm_gain, w_qkv, w_out, grad_out):
    full_width = layer_input.shape[1]
    head_count = N_GX * N_GY
    inputs_f = layer_input.astype(jnp.float32)
    inv_rms = lax.rsqrt(lax.optimization_barrier(jnp.mean(inputs_f * inputs_f, axis=1)) + epsilon)
    row_gain = jnp.where(modality[:, None] == 1, norm_gain[1][None, :], norm_gain[0][None, :])
    scaled = inputs_f * inv_rms[:, None]
    normed = (scaled * row_gain).astype(jnp.bfloat16)
    projected = [jnp.dot(normed, w_qkv[matrix_idx], preferred_element_type=jnp.float32).astype(jnp.bfloat16) for matrix_idx in range(3)]
    positions = jnp.arange(TOKENS, dtype=jnp.int32)
    span_ids = span_index(positions, image_spans)
    allowed = visible(positions, span_ids, positions, span_ids)
    d_attended = jnp.dot(grad_out, w_out.T, preferred_element_type=jnp.float32).astype(jnp.bfloat16)
    score_scale = 1.0 / math.sqrt(HEAD_DIM)

    def split_heads(matrix):
        return matrix.reshape(TOKENS, head_count, HEAD_DIM).transpose(1, 0, 2)

    def merge_heads(stacked):
        return stacked.transpose(1, 0, 2).reshape(TOKENS, head_count * HEAD_DIM)

    def one_head(operands):
        queries, keys, values, d_head = operands
        scores = jnp.dot(queries, keys.T, preferred_element_type=jnp.float32) * score_scale
        maxima = lax.optimization_barrier(jnp.max(jnp.where(allowed, scores, masked_low), axis=1))
        summed = lax.optimization_barrier(jnp.sum(jnp.where(allowed, jnp.exp(scores - maxima[:, None]), 0.0), axis=1))
        lse = maxima + jnp.log(summed)
        attn_p = jnp.where(allowed, jnp.exp(scores - lse[:, None]), 0.0)
        attn_pb = attn_p.astype(jnp.bfloat16)
        attended = jnp.dot(attn_pb, values, preferred_element_type=jnp.float32).astype(jnp.bfloat16)
        row_dots = lax.optimization_barrier(jnp.sum(d_head.astype(jnp.float32) * attended.astype(jnp.float32), axis=1))
        d_probs = jnp.dot(d_head, values.T, preferred_element_type=jnp.float32)
        d_scores = (attn_p * (d_probs - row_dots[:, None]) * score_scale).astype(jnp.bfloat16)
        d_queries = jnp.dot(d_scores, keys, preferred_element_type=jnp.float32).astype(jnp.bfloat16)
        score_blocks = d_scores.reshape(N_GZ, TOK_DEV, TOKENS).astype(jnp.float32)
        prob_blocks = attn_pb.reshape(N_GZ, TOK_DEV, TOKENS).astype(jnp.float32)
        query_blocks = queries.reshape(N_GZ, TOK_DEV, HEAD_DIM).astype(jnp.float32)
        upstream_blocks = d_head.reshape(N_GZ, TOK_DEV, HEAD_DIM).astype(jnp.float32)
        key_parts = jnp.einsum('gik,gid->gkd', score_blocks, query_blocks)
        value_parts = jnp.einsum('gik,gid->gkd', prob_blocks, upstream_blocks)
        d_keys = lax.optimization_barrier(jnp.sum(rounded(key_parts), axis=0)).astype(jnp.bfloat16)
        d_values = lax.optimization_barrier(jnp.sum(rounded(value_parts), axis=0)).astype(jnp.bfloat16)
        return (attended, d_queries, d_keys, d_values)
    results = lax.map(one_head, (split_heads(projected[0]), split_heads(projected[1]), split_heads(projected[2]), split_heads(d_attended)))
    attended = merge_heads(results[0])
    grads = [merge_heads(results[1]), merge_heads(results[2]), merge_heads(results[3])]
    branch = jnp.zeros((TOKENS, full_width), jnp.float32)
    grad_normed = jnp.zeros((TOKENS, full_width), jnp.float32)
    for head in range(head_count):
        columns = slice(head * HEAD_DIM, (head + 1) * HEAD_DIM)
        branch = branch + rounded(jnp.dot(attended[:, columns], w_out[columns], preferred_element_type=jnp.float32))
        partial_value = jnp.zeros((TOKENS, full_width), jnp.float32)
        for matrix_idx in range(3):
            partial_value = partial_value + jnp.dot(grads[matrix_idx][:, columns], w_qkv[matrix_idx][:, columns].T, preferred_element_type=jnp.float32)
        grad_normed = grad_normed + rounded(partial_value)
    attn_out = branch.astype(jnp.bfloat16)
    grad_wout = jnp.zeros((head_count * HEAD_DIM, full_width), jnp.float32)
    qkv_parts = [jnp.zeros((full_width, head_count * HEAD_DIM), jnp.float32) for matrix_idx in range(3)]
    for group in range(N_GZ):
        tok_rows = slice(group * TOK_DEV, (group + 1) * TOK_DEV)
        grad_wout = grad_wout + rounded(jnp.dot(attended[tok_rows].T, grad_out[tok_rows], preferred_element_type=jnp.float32))
        for matrix_idx in range(3):
            qkv_parts[matrix_idx] = qkv_parts[matrix_idx] + rounded(jnp.dot(normed[tok_rows].T, grads[matrix_idx][tok_rows], preferred_element_type=jnp.float32))
    grad_qkv = jnp.stack(qkv_parts)
    upstream = grad_normed * row_gain
    norm_dots = lax.optimization_barrier(jnp.mean(upstream * scaled, axis=1))
    grad_in = (inv_rms[:, None] * (upstream - scaled * norm_dots[:, None])).astype(jnp.bfloat16)
    onehot = (modality[:, None] == jnp.arange(2, dtype=jnp.int32)[None, :]).astype(jnp.float32)
    grad_gain = jnp.dot(onehot.T, grad_normed * scaled, precision=lax.Precision.HIGHEST)
    return (attn_out, grad_in, grad_qkv, grad_wout, grad_gain)
```

```python
import functools
import math

import jax
import jax.numpy as jnp
from jax import lax
from jax.sharding import PartitionSpec as P

epsilon = 1e-05
masked_low = -1e30


def span_index(positions, image_spans):
    inside = (positions[:, None] >= image_spans[0][None, :]) & (
        positions[:, None] < image_spans[1][None, :]
    )
    labels = jnp.arange(1, image_spans.shape[1] + 1, dtype=jnp.int32)
    return jnp.sum(jnp.where(inside, labels[None, :], 0), axis=1) - 1


def visible(query_pos, query_span, key_pos, key_span):
    causal = key_pos[None, :] <= query_pos[:, None]
    same_image = (query_span[:, None] == key_span[None, :]) & (query_span[:, None] >= 0)
    return causal | same_image


def shift_ring(block, step):
    count = lax.axis_size("gz")
    return lax.ppermute(block, "gz", [(src, (src + step) % count) for src in range(count)])


def ring_blocks(block):
    return [block] + [shift_ring(block, -step) for step in range(1, lax.axis_size("gz"))]


def ring_reduce(chunk_of):
    moved = [
        shift_ring(chunk_of(step).astype(jnp.bfloat16), step)
        for step in range(1, lax.axis_size("gz"))
    ]
    total = chunk_of(0)
    for term in moved:
        total = total + term.astype(jnp.float32)
    return total


def gather_features(block):
    return lax.all_gather(block, ("gx", "gy"), axis=1, tiled=True)


def per_device(layer_input, modality, image_spans, norm_gain, w_qkv, w_out, grad_out):
    f32, bf16 = jnp.float32, jnp.bfloat16
    tok_rows, local_width = layer_input.shape
    head_dim = w_qkv.shape[2]
    half = w_qkv.shape[1]
    count = lax.axis_size("gz")
    mine = lax.axis_index("gz")
    score_scale = 1.0 / math.sqrt(head_dim)
    owners = [lax.rem(mine + step, count) for step in range(count)]

    w_blocks = ring_blocks(w_qkv)
    wo_blocks = ring_blocks(w_out)
    x_full = gather_features(layer_input)
    gain_full = gather_features(norm_gain)
    go_full = gather_features(grad_out)
    full_width = x_full.shape[1]

    x_f = x_full.astype(f32)
    inv_rms = lax.rsqrt(jnp.sum(x_f * x_f, axis=1) / full_width + epsilon)
    picked = modality[:, None] == 1
    normed = (
        (x_f * inv_rms[:, None]) * jnp.where(picked, gain_full[1][None, :], gain_full[0][None, :])
    ).astype(bf16)

    def columns_of(matrix, step):
        return lax.dynamic_slice_in_dim(matrix, owners[step] * half, half, 1)

    projected = 0.0
    for step in range(count):
        projected = projected + jnp.einsum(
            "tc,mch->mth", columns_of(normed, step), w_blocks[step], preferred_element_type=f32
        )
    projected = projected.astype(bf16)
    queries = projected[0]
    kv_blocks = ring_blocks(jnp.concatenate([projected[1], projected[2]], axis=1))

    d_attended = 0.0
    for step in range(count):
        d_attended = d_attended + lax.dot_general(
            columns_of(go_full, step), wo_blocks[step], (((1,), (1,)), ((), ())),
            preferred_element_type=f32,
        )
    d_attended = d_attended.astype(bf16)

    local_pos = jnp.arange(tok_rows, dtype=jnp.int32)
    query_pos = mine * tok_rows + local_pos
    query_span = span_index(query_pos, image_spans)
    masked = []
    for step in range(count):
        key_pos = owners[step] * tok_rows + local_pos
        allowed = visible(query_pos, query_span, key_pos, span_index(key_pos, image_spans))
        scores = (
            lax.dot_general(
                queries, kv_blocks[step][:, :head_dim], (((1,), (1,)), ((), ())),
                preferred_element_type=f32,
            )
            * score_scale
        )
        masked.append(jnp.where(allowed, scores, masked_low))
    maxima = functools.reduce(jnp.maximum, [jnp.max(block, axis=1) for block in masked])
    summed = sum(jnp.sum(jnp.exp(block - maxima[:, None]), axis=1) for block in masked)
    lse = maxima + jnp.log(summed)
    probs = [jnp.exp(block - lse[:, None]) for block in masked]
    attended = sum(
        jnp.dot(probs[step].astype(bf16), kv_blocks[step][:, head_dim:], preferred_element_type=f32)
        for step in range(count)
    ).astype(bf16)

    all_heads = gather_features(attended)
    wo_rows = jnp.zeros((head_dim, full_width), bf16)
    for step in range(count):
        wo_rows = lax.dynamic_update_slice_in_dim(wo_rows, wo_blocks[step], owners[step] * half, 1)
    out_rows = lax.all_to_all(wo_rows, ("gx", "gy"), split_axis=1, concat_axis=0, tiled=True)
    attn_out = jnp.dot(all_heads, out_rows, preferred_element_type=f32).astype(bf16)

    grad_wout = ring_reduce(
        lambda step: lax.dot_general(
            attended, columns_of(go_full, step), (((0,), (0,)), ((), ())),
            preferred_element_type=f32,
        )
    )

    row_dots = jnp.sum(d_attended.astype(f32) * attended.astype(f32), axis=1)
    d_scores = []
    for step in range(count):
        d_probs = lax.dot_general(
            d_attended, kv_blocks[step][:, head_dim:], (((1,), (1,)), ((), ())),
            preferred_element_type=f32,
        )
        d_scores.append((probs[step] * (d_probs - row_dots[:, None]) * score_scale).astype(bf16))

    def kv_term(step):
        d_keys = lax.dot_general(
            d_scores[step], queries, (((0,), (0,)), ((), ())), preferred_element_type=f32
        )
        d_values = lax.dot_general(
            probs[step].astype(bf16), d_attended, (((0,), (0,)), ((), ())),
            preferred_element_type=f32,
        )
        return jnp.concatenate([d_keys, d_values], axis=1).astype(bf16).astype(f32)

    kv_grad = ring_reduce(kv_term)
    d_queries = sum(
        jnp.dot(d_scores[step], kv_blocks[step][:, :head_dim], preferred_element_type=f32)
        for step in range(count)
    )
    grads = jnp.stack([d_queries, kv_grad[:, :head_dim], kv_grad[:, head_dim:]]).astype(bf16)

    norm_dots = lax.psum(
        jnp.sum(grads.astype(f32) * projected.astype(f32), axis=(0, 2)), ("gx", "gy")
    )
    partial_rows = [
        jnp.einsum("mch,mth->ct", w_blocks[step], grads, preferred_element_type=f32).astype(bf16)
        for step in range(count)
    ]
    partial = jnp.zeros((full_width, tok_rows), bf16)
    for step in range(count):
        partial = lax.dynamic_update_slice_in_dim(partial, partial_rows[step], owners[step] * half, 0)
    grad_normed = (
        lax.psum_scatter(partial, ("gx", "gy"), scatter_dimension=0, tiled=True).astype(f32).T
    )
    grad_qkv = ring_reduce(
        lambda step: jnp.einsum(
            "tc,mth->mch", columns_of(normed, step), grads, preferred_element_type=f32
        )
    )

    row_gain = jnp.where(picked, norm_gain[1][None, :], norm_gain[0][None, :])
    scaled = layer_input.astype(f32) * inv_rms[:, None]
    upstream = grad_normed * row_gain
    grad_in = (inv_rms[:, None] * (upstream - scaled * (norm_dots / full_width)[:, None])).astype(
        bf16
    )
    weighted = grad_normed * scaled
    local_gain = jnp.stack(
        [
            jnp.sum(jnp.where(modality[:, None] == kind, weighted, 0.0), axis=0)
            for kind in range(norm_gain.shape[0])
        ]
    )
    if count == 2:
        grad_gain = local_gain + shift_ring(local_gain, 1)
    else:
        grad_gain = lax.psum(local_gain, "gz")
    return (attn_out, grad_in, grad_qkv, grad_wout, grad_gain)


def solution(mesh):
    in_specs = (
        P("gz", ("gx", "gy")),
        P("gz"),
        P(),
        P(None, ("gx", "gy")),
        P(None, "gz", ("gx", "gy")),
        P(("gx", "gy"), "gz"),
        P("gz", ("gx", "gy")),
    )
    out_specs = (
        P("gz", ("gx", "gy")),
        P("gz", ("gx", "gy")),
        P(None, "gz", ("gx", "gy")),
        P(("gx", "gy"), "gz"),
        P(None, ("gx", "gy")),
    )
    return jax.shard_map(
        per_device, mesh=mesh, in_specs=in_specs, out_specs=out_specs, check_vma=False
    )
```

```python
import functools
import math

import jax
import jax.numpy as jnp
from jax import lax
from jax.experimental import pallas as pl
from jax.experimental.pallas import tpu as pltpu
from jax.sharding import PartitionSpec as P

epsilon = 1e-05
masked_low = -1e30


def span_index(positions, image_spans):
    inside = (positions[:, None] >= image_spans[0][None, :]) & (
        positions[:, None] < image_spans[1][None, :]
    )
    labels = jnp.arange(1, image_spans.shape[1] + 1, dtype=jnp.int32)
    return jnp.sum(jnp.where(inside, labels[None, :], 0), axis=1) - 1


def visible(query_pos, query_span, key_pos, key_span):
    causal = key_pos[None, :] <= query_pos[:, None]
    same_image = (query_span[:, None] == key_span[None, :]) & (query_span[:, None] >= 0)
    return causal | same_image


MESH = pl.DeviceIdType.MESH


def place():
    gx, gy, gz = lax.axis_index("gx"), lax.axis_index("gy"), lax.axis_index("gz")
    return gx // 2, lax.rem(gx, 2), gy, gz


def greet(peers):
    barrier = pltpu.get_barrier_semaphore()
    for condition, device in peers:

        @pl.when(condition)
        def _():
            pl.semaphore_signal(barrier, inc=1, device_id=device, device_id_type=MESH)

    pl.semaphore_wait(barrier, sum(jnp.where(condition, 1, 0) for condition, _ in peers))


def remote(src, dst, send, recv, device):
    return pltpu.make_async_remote_copy(
        src_ref=src, dst_ref=dst, send_sem=send, recv_sem=recv, device_id=device,
        device_id_type=MESH,
    )


def gather_body(arity, nx, nz, *refs):
    ins, outs = refs[:arity], refs[arity : 2 * arity]
    line_send, line_recv, side_send, side_recv, core_send, core_recv = refs[2 * arity :]
    hi, lo, z, gz = place()
    pairs = nx // 2
    sides = [lax.rem(hi + r, pairs) for r in range(1, pairs)]
    partner = (hi * 2 + 1 - lo, z, gz)
    flows = [(1, z < nz - 1), (-1, z > 0)]

    def along(sign):
        return (hi * 2 + lo, z + sign, gz)

    def block(k, h, c, o):
        width = ins[k].shape[1]
        start = ((h * 2 + c) * nz + o) * width
        return outs[k].at[:, pl.ds(pl.multiple_of(start, width), width)]

    def line_copy(k, way, dist, src, o):
        return remote(
            src, block(k, hi, lo, o), line_send.at[k, way, dist], line_recv.at[k, way, dist + 1],
            along(flows[way][0]),
        )

    def spread(k, src, o):
        copies = [
            remote(
                src, block(k, hi, lo, o), side_send.at[k, r, o], side_recv.at[k, r, o],
                (sides[r] * 2 + lo, z, gz),
            )
            for r in range(pairs - 1)
        ]
        copies.append(core_copy(k, src, hi, o))
        return copies

    def core_copy(k, src, h, o):
        return remote(
            src, block(k, h, lo, o), core_send.at[k, h, o], core_recv.at[k, h, o], partner
        )

    greet(
        [(flows[0][1], along(1)), (flows[1][1], along(-1)), (z >= 0, partner)]
        + [(z >= 0, (side * 2 + lo, z, gz)) for side in sides]
    )
    for k in range(arity):
        for way in range(2):

            @pl.when(flows[way][1])
            def _():
                line_copy(k, way, 0, ins[k], z).start()

        for copy in spread(k, ins[k], z):
            copy.start()
        width = ins[k].shape[1]
        own = pl.ds(pl.multiple_of(((hi * 2 + lo) * nz + z) * width, width), width)
        outs[k][:, own] = ins[k][...]

    def side_arrivals(dist):
        for origin, valid in origins(dist):

            @pl.when(valid)
            def _():
                for k in range(arity):
                    for r in range(pairs - 1):
                        source = lax.rem(hi - r - 1 + pairs, pairs)
                        landed = block(k, source, lo, origin)
                        remote(
                            landed, landed, side_send.at[k, r, origin], side_recv.at[k, r, origin],
                            partner,
                        ).wait_recv()
                        core_copy(k, landed, source, origin).start()

    def origins(dist):
        if dist == 0:
            return [(z, z >= 0)]
        return [(z - dist, z - dist >= 0), (z + dist, z + dist < nz)]

    for dist in range(1, nz):
        for way, (origin, valid) in enumerate(origins(dist)):

            @pl.when(valid)
            def _():
                for k in range(arity):
                    landed = block(k, hi, lo, origin)
                    remote(
                        landed, landed, line_send.at[k, way, dist], line_recv.at[k, way, dist],
                        partner,
                    ).wait_recv()
                    if dist < nz - 1:

                        @pl.when(flows[way][1])
                        def _():
                            line_copy(k, way, dist, landed, origin).start()

                    for copy in spread(k, landed, origin):
                        copy.start()

        side_arrivals(dist - 1)
    side_arrivals(nz - 1)
    for k in range(arity):
        for o in range(nz):
            for h in range(pairs):
                landed = block(k, h, 1 - lo, o)
                waiting = remote(
                    landed, landed, core_send.at[k, h, o], core_recv.at[k, h, o], partner
                )
                waiting.wait_recv()
                waiting.wait_send()
            for r in range(pairs - 1):
                landed = block(k, hi, lo, o)
                remote(
                    landed, landed, side_send.at[k, r, o], side_recv.at[k, r, o], partner
                ).wait_send()
        for dist in range(nz - 1):
            for way in range(2):
                origin, valid = (z - dist, z - dist >= 0) if way == 0 else (z + dist, z + dist < nz)

                @pl.when(valid & flows[way][1])
                def _():
                    line_copy(k, way, dist, ins[k], z).wait_send()


def gather_kernel(arrays, collective_id):
    nx, nz = lax.axis_size("gx"), lax.axis_size("gy")
    arity, pairs = len(arrays), nx // 2
    dma = pltpu.SemaphoreType.DMA
    vmem = pl.BlockSpec(memory_space=pltpu.VMEM)
    return pl.pallas_call(
        functools.partial(gather_body, arity, nx, nz),
        out_shape=[
            jax.ShapeDtypeStruct((a.shape[0], a.shape[1] * nx * nz), a.dtype) for a in arrays
        ],
        in_specs=[vmem] * arity,
        out_specs=[vmem] * arity,
        scratch_shapes=[
            dma((arity, 2, nz)), dma((arity, 2, nz)),
            dma((arity, max(pairs - 1, 1), nz)), dma((arity, max(pairs - 1, 1), nz)),
            dma((arity, pairs, nz)), dma((arity, pairs, nz)),
        ],
        compiler_params=pltpu.CompilerParams(collective_id=collective_id, has_side_effects=True),
        cost_estimate=pl.CostEstimate(
            flops=sum(a.size * a.dtype.itemsize for a in arrays) * 80000, bytes_accessed=2**23,
            transcendentals=0,
        ),
        name="gather_features",
    )(*arrays)


def reduce_body(
    nx, nz, part, dots, out, dots_out, cbuf, csum, xbuf, lbuf, lsend, acc, dbuf, dsum,
    core_send, core_recv, side_send, side_recv, line_send, line_recv, dot_send, dot_recv,
):
    hi, lo, z, gz = place()
    pairs = nx // 2
    width = out.shape[1]
    f32 = jnp.float32
    sides = [lax.rem(hi + r, pairs) for r in range(1, pairs)]
    partner = (hi * 2 + 1 - lo, z, gz)
    flows = [(1, z < nz - 1), (-1, z > 0)]
    depth = [(hi * 2 + lo, lax.rem(z + r, nz), gz) for r in range(1, nz)]

    def columns(h, c, o):
        return pl.ds(pl.multiple_of(((h * 2 + c) * nz + o) * width, width), width)

    def along(sign):
        return (hi * 2 + lo, z + sign, gz)

    def targets():
        for dist in range(nz - 1, 0, -1):
            yield 0, dist, z + dist, z + dist < nz
            yield 1, dist, z - dist, z - dist >= 0

    def core_copy(h, o):
        return remote(
            part.at[:, columns(h, 1 - lo, o)], cbuf.at[h, o], core_send.at[h, o],
            core_recv.at[h, o], partner,
        )

    def side_copy(r, o):
        return remote(
            csum.at[r, o], xbuf.at[r, o], side_send.at[r, o], side_recv.at[r, o],
            (sides[r] * 2 + lo, z, gz),
        )

    def line_copy(way, dist):
        return remote(
            lsend.at[way, dist - 1], lbuf.at[way, dist - 1], line_send.at[way, dist - 1],
            line_recv.at[way, dist - 1], along(flows[way][0]),
        )

    def dot_copy(src, slot, device):
        return remote(src, dbuf.at[slot], dot_send.at[slot], dot_recv.at[slot], device)

    greet(
        [(z >= 0, partner)]
        + [(z >= 0, (side * 2 + lo, z, gz)) for side in sides]
        + [(z >= 0, device) for device in depth]
    )
    order = list(targets()) + [(0, 0, z, z >= 0)]
    for way, dist, o, valid in order:

        @pl.when(valid)
        def _():
            for side in sides:
                core_copy(side, o).start()
            core_copy(hi, o).start()

    dot_first = dot_copy(dots, 0, partner)
    dot_first.start()
    for way, dist, o, valid in order:

        @pl.when(valid)
        def _():
            for r, side in enumerate(sides):
                core_copy(side, o).wait_recv()
                csum[r, o] = (
                    part[:, columns(side, lo, o)].astype(f32) + cbuf[side, o].astype(f32)
                ).astype(csum.dtype)
                side_copy(r, o).start()

    dot_first.wait_recv()
    dsum[0] = dots[...] + dbuf[0]
    dot_sides = [
        dot_copy(dsum.at[0], 1 + r, (sides[r] * 2 + lo, z, gz)) for r in range(pairs - 1)
    ]
    for copy in dot_sides:
        copy.start()

    def merge(o):
        core_copy(hi, o).wait_recv()
        total = part[:, columns(hi, lo, o)].astype(f32) + cbuf[hi, o].astype(f32)
        for r in range(pairs - 1):
            side_copy(r, o).wait_recv()
            total = total + xbuf[r, o].astype(f32)
        acc[...] = total

    def add_line(way, dist):
        source = flows[1 - way]

        @pl.when(source[1])
        def _():
            remote(
                lbuf.at[way, dist], lbuf.at[way, dist], line_send.at[way, dist],
                line_recv.at[way, dist], partner,
            ).wait_recv()
            acc[...] += lbuf[way, dist].astype(f32)

    for way, dist, o, valid in targets():

        @pl.when(valid)
        def _():
            merge(o)
            if dist < nz - 1:
                add_line(way, dist)
            lsend[way, dist - 1] = acc[...].astype(lsend.dtype)
            line_copy(way, dist).start()

    dots_now = dsum[0]
    for r, copy in enumerate(dot_sides):
        copy.wait_recv()
        dots_now = dots_now + dbuf[1 + r]
    dsum[1] = dots_now
    dot_depth = [dot_copy(dsum.at[1], pairs + r, depth[r]) for r in range(nz - 1)]
    for copy in dot_depth:
        copy.start()
    merge(z)
    if nz > 1:
        add_line(0, 0)
        add_line(1, 0)
    out[...] = acc[...]
    for r, copy in enumerate(dot_depth):
        copy.wait_recv()
        dots_now = dots_now + dbuf[pairs + r]
    dots_out[...] = dots_now
    for copy in [dot_first] + dot_sides + dot_depth:
        copy.wait_send()
    for o in range(nz):
        for h in range(pairs):
            core_copy(h, o).wait_send()
        for r in range(pairs - 1):
            side_copy(r, o).wait_send()
    for way, dist, o, valid in targets():

        @pl.when(valid)
        def _():
            line_copy(way, dist).wait_send()


def reduce_kernel(part, dots, collective_id):
    nx, nz = lax.axis_size("gx"), lax.axis_size("gy")
    pairs = nx // 2
    rows, width = part.shape[0], part.shape[1] // (nx * nz)
    dots = dots.reshape(-1, 128)
    dma = pltpu.SemaphoreType.DMA
    vmem = pl.BlockSpec(memory_space=pltpu.VMEM)
    others, line = max(pairs - 1, 1), max(nz - 1, 1)
    tile = (rows, width)
    summed, dots_total = pl.pallas_call(
        functools.partial(reduce_body, nx, nz),
        out_shape=[
            jax.ShapeDtypeStruct(tile, jnp.float32),
            jax.ShapeDtypeStruct(dots.shape, jnp.float32),
        ],
        in_specs=[vmem] * 2,
        out_specs=[vmem] * 2,
        scratch_shapes=[
            pltpu.VMEM((pairs, nz) + tile, part.dtype),
            pltpu.VMEM((others, nz) + tile, part.dtype),
            pltpu.VMEM((others, nz) + tile, part.dtype),
            pltpu.VMEM((2, line) + tile, part.dtype),
            pltpu.VMEM((2, line) + tile, part.dtype),
            pltpu.VMEM(tile, jnp.float32),
            pltpu.VMEM((pairs + line,) + dots.shape, jnp.float32),
            pltpu.VMEM((2,) + dots.shape, jnp.float32),
            dma((pairs, nz)), dma((pairs, nz)),
            dma((others, nz)), dma((others, nz)),
            dma((2, line)), dma((2, line)),
            dma((pairs + line,)), dma((pairs + line,)),
        ],
        compiler_params=pltpu.CompilerParams(collective_id=collective_id, has_side_effects=True),
        cost_estimate=pl.CostEstimate(
            flops=part.size * 12000, bytes_accessed=2**23, transcendentals=0
        ),
        name="reduce_features",
    )(part, dots)
    return summed, dots_total.reshape(-1)


def shift_ring(block, step):
    count = lax.axis_size("gz")
    return lax.ppermute(block, "gz", [(src, (src + step) % count) for src in range(count)])


def ring_blocks(block):
    return [block] + [shift_ring(block, -step) for step in range(1, lax.axis_size("gz"))]


def ring_reduce(chunk_of):
    moved = [
        shift_ring(chunk_of(step).astype(jnp.bfloat16), step)
        for step in range(1, lax.axis_size("gz"))
    ]
    total = chunk_of(0)
    for term in moved:
        total = total + term.astype(jnp.float32)
    return total


def gather_features(block):
    return lax.all_gather(block, ("gx", "gy"), axis=1, tiled=True)


def per_device(layer_input, modality, image_spans, norm_gain, w_qkv, w_out, grad_out):
    f32, bf16 = jnp.float32, jnp.bfloat16
    tok_rows, local_width = layer_input.shape
    head_dim = w_qkv.shape[2]
    half = w_qkv.shape[1]
    count = lax.axis_size("gz")
    mine = lax.axis_index("gz")
    score_scale = 1.0 / math.sqrt(head_dim)
    owners = [lax.rem(mine + step, count) for step in range(count)]

    w_blocks = ring_blocks(w_qkv)
    wo_blocks = ring_blocks(w_out)
    x_full, gain_full = gather_kernel([layer_input, norm_gain], 1)
    go_full = gather_features(grad_out)
    full_width = x_full.shape[1]

    x_f = x_full.astype(f32)
    inv_rms = lax.rsqrt(jnp.sum(x_f * x_f, axis=1) / full_width + epsilon)
    picked = modality[:, None] == 1
    normed = (
        (x_f * inv_rms[:, None]) * jnp.where(picked, gain_full[1][None, :], gain_full[0][None, :])
    ).astype(bf16)

    def columns_of(matrix, step):
        return lax.dynamic_slice_in_dim(matrix, owners[step] * half, half, 1)

    projected = 0.0
    for step in range(count):
        projected = projected + jnp.einsum(
            "tc,mch->mth", columns_of(normed, step), w_blocks[step], preferred_element_type=f32
        )
    projected = projected.astype(bf16)
    queries = projected[0]
    kv_blocks = ring_blocks(jnp.concatenate([projected[1], projected[2]], axis=1))

    d_attended = 0.0
    for step in range(count):
        d_attended = d_attended + lax.dot_general(
            columns_of(go_full, step), wo_blocks[step], (((1,), (1,)), ((), ())),
            preferred_element_type=f32,
        )
    d_attended = d_attended.astype(bf16)

    local_pos = jnp.arange(tok_rows, dtype=jnp.int32)
    query_pos = mine * tok_rows + local_pos
    query_span = span_index(query_pos, image_spans)
    masked = []
    for step in range(count):
        key_pos = owners[step] * tok_rows + local_pos
        allowed = visible(query_pos, query_span, key_pos, span_index(key_pos, image_spans))
        scores = (
            lax.dot_general(
                queries, kv_blocks[step][:, :head_dim], (((1,), (1,)), ((), ())),
                preferred_element_type=f32,
            )
            * score_scale
        )
        masked.append(jnp.where(allowed, scores, masked_low))
    maxima = functools.reduce(jnp.maximum, [jnp.max(block, axis=1) for block in masked])
    summed = sum(jnp.sum(jnp.exp(block - maxima[:, None]), axis=1) for block in masked)
    lse = maxima + jnp.log(summed)
    probs = [jnp.exp(block - lse[:, None]) for block in masked]
    attended = sum(
        jnp.dot(probs[step].astype(bf16), kv_blocks[step][:, head_dim:], preferred_element_type=f32)
        for step in range(count)
    ).astype(bf16)

    all_heads = gather_features(attended)
    wo_rows = jnp.zeros((head_dim, full_width), bf16)
    for step in range(count):
        wo_rows = lax.dynamic_update_slice_in_dim(wo_rows, wo_blocks[step], owners[step] * half, 1)
    out_rows = lax.all_to_all(wo_rows, ("gx", "gy"), split_axis=1, concat_axis=0, tiled=True)
    attn_out = jnp.dot(all_heads, out_rows, preferred_element_type=f32).astype(bf16)

    grad_wout = ring_reduce(
        lambda step: lax.dot_general(
            attended, columns_of(go_full, step), (((0,), (0,)), ((), ())),
            preferred_element_type=f32,
        )
    )

    row_dots = jnp.sum(d_attended.astype(f32) * attended.astype(f32), axis=1)
    d_scores = []
    for step in range(count):
        d_probs = lax.dot_general(
            d_attended, kv_blocks[step][:, head_dim:], (((1,), (1,)), ((), ())),
            preferred_element_type=f32,
        )
        d_scores.append((probs[step] * (d_probs - row_dots[:, None]) * score_scale).astype(bf16))

    def kv_term(step):
        d_keys = lax.dot_general(
            d_scores[step], queries, (((0,), (0,)), ((), ())), preferred_element_type=f32
        )
        d_values = lax.dot_general(
            probs[step].astype(bf16), d_attended, (((0,), (0,)), ((), ())),
            preferred_element_type=f32,
        )
        return jnp.concatenate([d_keys, d_values], axis=1).astype(bf16).astype(f32)

    kv_grad = ring_reduce(kv_term)
    d_queries = sum(
        jnp.dot(d_scores[step], kv_blocks[step][:, :head_dim], preferred_element_type=f32)
        for step in range(count)
    )
    grads = jnp.stack([d_queries, kv_grad[:, :head_dim], kv_grad[:, head_dim:]]).astype(bf16)

    dots = jnp.sum(grads.astype(f32) * projected.astype(f32), axis=(0, 2))
    partial = jnp.zeros((tok_rows, full_width), bf16)
    for step in range(count):
        partial = lax.dynamic_update_slice_in_dim(
            partial,
            jnp.einsum(
                "mth,mch->tc", grads, w_blocks[step], preferred_element_type=f32
            ).astype(bf16),
            owners[step] * half,
            1,
        )
    grad_normed, norm_dots = reduce_kernel(partial, dots, 2)
    grad_qkv = ring_reduce(
        lambda step: jnp.einsum(
            "tc,mth->mch", columns_of(normed, step), grads, preferred_element_type=f32
        )
    )

    row_gain = jnp.where(picked, norm_gain[1][None, :], norm_gain[0][None, :])
    scaled = layer_input.astype(f32) * inv_rms[:, None]
    upstream = grad_normed * row_gain
    grad_in = (inv_rms[:, None] * (upstream - scaled * (norm_dots / full_width)[:, None])).astype(
        bf16
    )
    weighted = grad_normed * scaled
    local_gain = jnp.stack(
        [
            jnp.sum(jnp.where(modality[:, None] == kind, weighted, 0.0), axis=0)
            for kind in range(norm_gain.shape[0])
        ]
    )
    if count == 2:
        grad_gain = local_gain + shift_ring(local_gain, 1)
    else:
        grad_gain = lax.psum(local_gain, "gz")
    return (attn_out, grad_in, grad_qkv, grad_wout, grad_gain)


def solution(mesh):
    in_specs = (
        P("gz", ("gx", "gy")),
        P("gz"),
        P(),
        P(None, ("gx", "gy")),
        P(None, "gz", ("gx", "gy")),
        P(("gx", "gy"), "gz"),
        P("gz", ("gx", "gy")),
    )
    out_specs = (
        P("gz", ("gx", "gy")),
        P("gz", ("gx", "gy")),
        P(None, "gz", ("gx", "gy")),
        P(("gx", "gy"), "gz"),
        P(None, ("gx", "gy")),
    )
    return jax.shard_map(
        per_device, mesh=mesh, in_specs=in_specs, out_specs=out_specs, check_vma=False
    )
```

```python
import functools
import math

import jax
import jax.numpy as jnp
from jax import lax
from jax.experimental import pallas as pl
from jax.experimental.pallas import tpu as pltpu
from jax.sharding import PartitionSpec as P

epsilon = 1e-05
masked_low = -1e30


def span_index(positions, image_spans):
    inside = (positions[:, None] >= image_spans[0][None, :]) & (
        positions[:, None] < image_spans[1][None, :]
    )
    labels = jnp.arange(1, image_spans.shape[1] + 1, dtype=jnp.int32)
    return jnp.sum(jnp.where(inside, labels[None, :], 0), axis=1) - 1


def visible(query_pos, query_span, key_pos, key_span):
    causal = key_pos[None, :] <= query_pos[:, None]
    same_image = (query_span[:, None] == key_span[None, :]) & (query_span[:, None] >= 0)
    return causal | same_image


MESH = pl.DeviceIdType.MESH


def place():
    gx, gy, gz = lax.axis_index("gx"), lax.axis_index("gy"), lax.axis_index("gz")
    return gx // 2, lax.rem(gx, 2), gy, gz


def greet(peers):
    barrier = pltpu.get_barrier_semaphore()
    for condition, device in peers:

        @pl.when(condition)
        def _():
            pl.semaphore_signal(barrier, inc=1, device_id=device, device_id_type=MESH)

    pl.semaphore_wait(barrier, sum(jnp.where(condition, 1, 0) for condition, _ in peers))


def remote(src, dst, send, recv, device):
    return pltpu.make_async_remote_copy(
        src_ref=src, dst_ref=dst, send_sem=send, recv_sem=recv, device_id=device,
        device_id_type=MESH,
    )


def gather_body(arity, nx, nz, *refs):
    ins, outs = refs[:arity], refs[arity : 2 * arity]
    line_send, line_recv, side_send, side_recv, core_send, core_recv = refs[2 * arity :]
    hi, lo, z, gz = place()
    pairs = nx // 2
    sides = [lax.rem(hi + r, pairs) for r in range(1, pairs)]
    partner = (hi * 2 + 1 - lo, z, gz)
    flows = [(1, z < nz - 1), (-1, z > 0)]

    def along(sign):
        return (hi * 2 + lo, z + sign, gz)

    def block(k, h, c, o):
        width = ins[k].shape[1]
        start = ((h * 2 + c) * nz + o) * width
        return outs[k].at[:, pl.ds(pl.multiple_of(start, width), width)]

    def line_copy(k, way, dist, src, o):
        return remote(
            src, block(k, hi, lo, o), line_send.at[k, way, dist], line_recv.at[k, way, dist + 1],
            along(flows[way][0]),
        )

    def spread(k, src, o):
        copies = [
            remote(
                src, block(k, hi, lo, o), side_send.at[k, r, o], side_recv.at[k, r, o],
                (sides[r] * 2 + lo, z, gz),
            )
            for r in range(pairs - 1)
        ]
        copies.append(core_copy(k, src, hi, o))
        return copies

    def core_copy(k, src, h, o):
        return remote(
            src, block(k, h, lo, o), core_send.at[k, h, o], core_recv.at[k, h, o], partner
        )

    greet(
        [(flows[0][1], along(1)), (flows[1][1], along(-1)), (z >= 0, partner)]
        + [(z >= 0, (side * 2 + lo, z, gz)) for side in sides]
    )
    for k in range(arity):
        for way in range(2):

            @pl.when(flows[way][1])
            def _():
                line_copy(k, way, 0, ins[k], z).start()

        for copy in spread(k, ins[k], z):
            copy.start()
        width = ins[k].shape[1]
        own = pl.ds(pl.multiple_of(((hi * 2 + lo) * nz + z) * width, width), width)
        outs[k][:, own] = ins[k][...]

    def side_arrivals(dist):
        for origin, valid in origins(dist):

            @pl.when(valid)
            def _():
                for k in range(arity):
                    for r in range(pairs - 1):
                        source = lax.rem(hi - r - 1 + pairs, pairs)
                        landed = block(k, source, lo, origin)
                        remote(
                            landed, landed, side_send.at[k, r, origin], side_recv.at[k, r, origin],
                            partner,
                        ).wait_recv()
                        core_copy(k, landed, source, origin).start()

    def origins(dist):
        if dist == 0:
            return [(z, z >= 0)]
        return [(z - dist, z - dist >= 0), (z + dist, z + dist < nz)]

    for dist in range(1, nz):
        for way, (origin, valid) in enumerate(origins(dist)):

            @pl.when(valid)
            def _():
                for k in range(arity):
                    landed = block(k, hi, lo, origin)
                    remote(
                        landed, landed, line_send.at[k, way, dist], line_recv.at[k, way, dist],
                        partner,
                    ).wait_recv()
                    if dist < nz - 1:

                        @pl.when(flows[way][1])
                        def _():
                            line_copy(k, way, dist, landed, origin).start()

                    for copy in spread(k, landed, origin):
                        copy.start()

        side_arrivals(dist - 1)
    side_arrivals(nz - 1)
    for k in range(arity):
        for o in range(nz):
            for h in range(pairs):
                landed = block(k, h, 1 - lo, o)
                waiting = remote(
                    landed, landed, core_send.at[k, h, o], core_recv.at[k, h, o], partner
                )
                waiting.wait_recv()
                waiting.wait_send()
            for r in range(pairs - 1):
                landed = block(k, hi, lo, o)
                remote(
                    landed, landed, side_send.at[k, r, o], side_recv.at[k, r, o], partner
                ).wait_send()
        for dist in range(nz - 1):
            for way in range(2):
                origin, valid = (z - dist, z - dist >= 0) if way == 0 else (z + dist, z + dist < nz)

                @pl.when(valid & flows[way][1])
                def _():
                    line_copy(k, way, dist, ins[k], z).wait_send()


def gather_kernel(arrays, collective_id):
    nx, nz = lax.axis_size("gx"), lax.axis_size("gy")
    arity, pairs = len(arrays), nx // 2
    dma = pltpu.SemaphoreType.DMA
    vmem = pl.BlockSpec(memory_space=pltpu.VMEM)
    return pl.pallas_call(
        functools.partial(gather_body, arity, nx, nz),
        out_shape=[
            jax.ShapeDtypeStruct((a.shape[0], a.shape[1] * nx * nz), a.dtype) for a in arrays
        ],
        in_specs=[vmem] * arity,
        out_specs=[vmem] * arity,
        scratch_shapes=[
            dma((arity, 2, nz)), dma((arity, 2, nz)),
            dma((arity, max(pairs - 1, 1), nz)), dma((arity, max(pairs - 1, 1), nz)),
            dma((arity, pairs, nz)), dma((arity, pairs, nz)),
        ],
        compiler_params=pltpu.CompilerParams(collective_id=collective_id, has_side_effects=True),
        cost_estimate=pl.CostEstimate(
            flops=sum(a.size * a.dtype.itemsize for a in arrays) * 80000, bytes_accessed=2**23,
            transcendentals=0,
        ),
        name="gather_features",
    )(*arrays)


def reduce_body(
    nx, nz, part, dots, out, dots_out, cbuf, csum, xbuf, lbuf, lsend, acc, dbuf, dsum,
    core_send, core_recv, side_send, side_recv, line_send, line_recv, dot_send, dot_recv,
):
    hi, lo, z, gz = place()
    pairs = nx // 2
    width = out.shape[1]
    f32 = jnp.float32
    sides = [lax.rem(hi + r, pairs) for r in range(1, pairs)]
    partner = (hi * 2 + 1 - lo, z, gz)
    flows = [(1, z < nz - 1), (-1, z > 0)]
    depth = [(hi * 2 + lo, lax.rem(z + r, nz), gz) for r in range(1, nz)]

    def columns(h, c, o):
        return pl.ds(pl.multiple_of(((h * 2 + c) * nz + o) * width, width), width)

    def along(sign):
        return (hi * 2 + lo, z + sign, gz)

    def targets():
        for dist in range(nz - 1, 0, -1):
            yield 0, dist, z + dist, z + dist < nz
            yield 1, dist, z - dist, z - dist >= 0

    def core_copy(h, o):
        return remote(
            part.at[:, columns(h, 1 - lo, o)], cbuf.at[h, o], core_send.at[h, o],
            core_recv.at[h, o], partner,
        )

    def side_copy(r, o):
        return remote(
            csum.at[r, o], xbuf.at[r, o], side_send.at[r, o], side_recv.at[r, o],
            (sides[r] * 2 + lo, z, gz),
        )

    def line_copy(way, dist):
        return remote(
            lsend.at[way, dist - 1], lbuf.at[way, dist - 1], line_send.at[way, dist - 1],
            line_recv.at[way, dist - 1], along(flows[way][0]),
        )

    def dot_copy(src, slot, device):
        return remote(src, dbuf.at[slot], dot_send.at[slot], dot_recv.at[slot], device)

    greet(
        [(z >= 0, partner)]
        + [(z >= 0, (side * 2 + lo, z, gz)) for side in sides]
        + [(z >= 0, device) for device in depth]
    )
    order = list(targets()) + [(0, 0, z, z >= 0)]
    for way, dist, o, valid in order:

        @pl.when(valid)
        def _():
            for side in sides:
                core_copy(side, o).start()
            core_copy(hi, o).start()

    dot_first = dot_copy(dots, 0, partner)
    dot_first.start()
    for way, dist, o, valid in order:

        @pl.when(valid)
        def _():
            for r, side in enumerate(sides):
                core_copy(side, o).wait_recv()
                csum[r, o] = (
                    part[:, columns(side, lo, o)].astype(f32) + cbuf[side, o].astype(f32)
                ).astype(csum.dtype)
                side_copy(r, o).start()

    dot_first.wait_recv()
    dsum[0] = dots[...] + dbuf[0]
    dot_sides = [
        dot_copy(dsum.at[0], 1 + r, (sides[r] * 2 + lo, z, gz)) for r in range(pairs - 1)
    ]
    for copy in dot_sides:
        copy.start()

    def merge(o):
        core_copy(hi, o).wait_recv()
        total = part[:, columns(hi, lo, o)].astype(f32) + cbuf[hi, o].astype(f32)
        for r in range(pairs - 1):
            side_copy(r, o).wait_recv()
            total = total + xbuf[r, o].astype(f32)
        acc[...] = total

    def add_line(way, dist):
        source = flows[1 - way]

        @pl.when(source[1])
        def _():
            remote(
                lbuf.at[way, dist], lbuf.at[way, dist], line_send.at[way, dist],
                line_recv.at[way, dist], partner,
            ).wait_recv()
            acc[...] += lbuf[way, dist].astype(f32)

    for way, dist, o, valid in targets():

        @pl.when(valid)
        def _():
            merge(o)
            if dist < nz - 1:
                add_line(way, dist)
            lsend[way, dist - 1] = acc[...].astype(lsend.dtype)
            line_copy(way, dist).start()

    dots_now = dsum[0]
    for r, copy in enumerate(dot_sides):
        copy.wait_recv()
        dots_now = dots_now + dbuf[1 + r]
    dsum[1] = dots_now
    dot_depth = [dot_copy(dsum.at[1], pairs + r, depth[r]) for r in range(nz - 1)]
    for copy in dot_depth:
        copy.start()
    merge(z)
    if nz > 1:
        add_line(0, 0)
        add_line(1, 0)
    out[...] = acc[...]
    for r, copy in enumerate(dot_depth):
        copy.wait_recv()
        dots_now = dots_now + dbuf[pairs + r]
    dots_out[...] = dots_now
    for copy in [dot_first] + dot_sides + dot_depth:
        copy.wait_send()
    for o in range(nz):
        for h in range(pairs):
            core_copy(h, o).wait_send()
        for r in range(pairs - 1):
            side_copy(r, o).wait_send()
    for way, dist, o, valid in targets():

        @pl.when(valid)
        def _():
            line_copy(way, dist).wait_send()


def reduce_kernel(part, dots, collective_id):
    nx, nz = lax.axis_size("gx"), lax.axis_size("gy")
    pairs = nx // 2
    rows, width = part.shape[0], part.shape[1] // (nx * nz)
    dots = dots.reshape(-1, 128)
    dma = pltpu.SemaphoreType.DMA
    vmem = pl.BlockSpec(memory_space=pltpu.VMEM)
    others, line = max(pairs - 1, 1), max(nz - 1, 1)
    tile = (rows, width)
    summed, dots_total = pl.pallas_call(
        functools.partial(reduce_body, nx, nz),
        out_shape=[
            jax.ShapeDtypeStruct(tile, jnp.float32),
            jax.ShapeDtypeStruct(dots.shape, jnp.float32),
        ],
        in_specs=[vmem] * 2,
        out_specs=[vmem] * 2,
        scratch_shapes=[
            pltpu.VMEM((pairs, nz) + tile, part.dtype),
            pltpu.VMEM((others, nz) + tile, part.dtype),
            pltpu.VMEM((others, nz) + tile, part.dtype),
            pltpu.VMEM((2, line) + tile, part.dtype),
            pltpu.VMEM((2, line) + tile, part.dtype),
            pltpu.VMEM(tile, jnp.float32),
            pltpu.VMEM((pairs + line,) + dots.shape, jnp.float32),
            pltpu.VMEM((2,) + dots.shape, jnp.float32),
            dma((pairs, nz)), dma((pairs, nz)),
            dma((others, nz)), dma((others, nz)),
            dma((2, line)), dma((2, line)),
            dma((pairs + line,)), dma((pairs + line,)),
        ],
        compiler_params=pltpu.CompilerParams(collective_id=collective_id, has_side_effects=True),
        cost_estimate=pl.CostEstimate(
            flops=part.size * 12000, bytes_accessed=2**23, transcendentals=0
        ),
        name="reduce_features",
    )(part, dots)
    return summed, dots_total.reshape(-1)


def shift_ring(block, step):
    count = lax.axis_size("gz")
    return lax.ppermute(block, "gz", [(src, (src + step) % count) for src in range(count)])


def ring_blocks(block):
    return [block] + [shift_ring(block, -step) for step in range(1, lax.axis_size("gz"))]


def ring_reduce(chunk_of):
    moved = [
        shift_ring(chunk_of(step).astype(jnp.bfloat16), step)
        for step in range(1, lax.axis_size("gz"))
    ]
    total = chunk_of(0)
    for term in moved:
        total = total + term.astype(jnp.float32)
    return total


def per_device(layer_input, modality, image_spans, norm_gain, w_qkv, w_out, grad_out):
    f32, bf16 = jnp.float32, jnp.bfloat16
    tok_rows, local_width = layer_input.shape
    head_dim = w_qkv.shape[2]
    half = w_qkv.shape[1]
    count = lax.axis_size("gz")
    mine = lax.axis_index("gz")
    score_scale = 1.0 / math.sqrt(head_dim)
    owners = [lax.rem(mine + step, count) for step in range(count)]

    w_blocks = ring_blocks(w_qkv)
    wo_blocks = ring_blocks(w_out)
    x_full, gain_full, go_full = gather_kernel([layer_input, norm_gain, grad_out], 1)
    full_width = x_full.shape[1]

    x_f = x_full.astype(f32)
    inv_rms = lax.rsqrt(jnp.sum(x_f * x_f, axis=1) / full_width + epsilon)
    picked = modality[:, None] == 1
    normed = (
        (x_f * inv_rms[:, None]) * jnp.where(picked, gain_full[1][None, :], gain_full[0][None, :])
    ).astype(bf16)

    def columns_of(matrix, step):
        return lax.dynamic_slice_in_dim(matrix, owners[step] * half, half, 1)

    projected = 0.0
    for step in range(count):
        projected = projected + jnp.einsum(
            "tc,mch->mth", columns_of(normed, step), w_blocks[step], preferred_element_type=f32
        )
    projected = projected.astype(bf16)
    queries = projected[0]
    kv_blocks = ring_blocks(jnp.concatenate([projected[1], projected[2]], axis=1))

    d_attended = 0.0
    for step in range(count):
        d_attended = d_attended + lax.dot_general(
            columns_of(go_full, step), wo_blocks[step], (((1,), (1,)), ((), ())),
            preferred_element_type=f32,
        )
    d_attended = d_attended.astype(bf16)

    local_pos = jnp.arange(tok_rows, dtype=jnp.int32)
    query_pos = mine * tok_rows + local_pos
    query_span = span_index(query_pos, image_spans)
    masked = []
    for step in range(count):
        key_pos = owners[step] * tok_rows + local_pos
        allowed = visible(query_pos, query_span, key_pos, span_index(key_pos, image_spans))
        scores = (
            lax.dot_general(
                queries, kv_blocks[step][:, :head_dim], (((1,), (1,)), ((), ())),
                preferred_element_type=f32,
            )
            * score_scale
        )
        masked.append(jnp.where(allowed, scores, masked_low))
    maxima = functools.reduce(jnp.maximum, [jnp.max(block, axis=1) for block in masked])
    summed = sum(jnp.sum(jnp.exp(block - maxima[:, None]), axis=1) for block in masked)
    lse = maxima + jnp.log(summed)
    probs = [jnp.exp(block - lse[:, None]) for block in masked]
    attended = sum(
        jnp.dot(probs[step].astype(bf16), kv_blocks[step][:, head_dim:], preferred_element_type=f32)
        for step in range(count)
    ).astype(bf16)

    (all_heads,) = gather_kernel([attended], 3)
    wo_rows = jnp.zeros((head_dim, full_width), bf16)
    for step in range(count):
        wo_rows = lax.dynamic_update_slice_in_dim(wo_rows, wo_blocks[step], owners[step] * half, 1)
    out_rows = lax.all_to_all(wo_rows, ("gx", "gy"), split_axis=1, concat_axis=0, tiled=True)
    attn_out = jnp.dot(all_heads, out_rows, preferred_element_type=f32).astype(bf16)

    grad_wout = ring_reduce(
        lambda step: lax.dot_general(
            attended, columns_of(go_full, step), (((0,), (0,)), ((), ())),
            preferred_element_type=f32,
        )
    )

    row_dots = jnp.sum(d_attended.astype(f32) * attended.astype(f32), axis=1)
    d_scores = []
    for step in range(count):
        d_probs = lax.dot_general(
            d_attended, kv_blocks[step][:, head_dim:], (((1,), (1,)), ((), ())),
            preferred_element_type=f32,
        )
        d_scores.append((probs[step] * (d_probs - row_dots[:, None]) * score_scale).astype(bf16))

    def kv_term(step):
        d_keys = lax.dot_general(
            d_scores[step], queries, (((0,), (0,)), ((), ())), preferred_element_type=f32
        )
        d_values = lax.dot_general(
            probs[step].astype(bf16), d_attended, (((0,), (0,)), ((), ())),
            preferred_element_type=f32,
        )
        return jnp.concatenate([d_keys, d_values], axis=1).astype(bf16).astype(f32)

    kv_grad = ring_reduce(kv_term)
    d_queries = sum(
        jnp.dot(d_scores[step], kv_blocks[step][:, :head_dim], preferred_element_type=f32)
        for step in range(count)
    )
    grads = jnp.stack([d_queries, kv_grad[:, :head_dim], kv_grad[:, head_dim:]]).astype(bf16)

    dots = jnp.sum(grads.astype(f32) * projected.astype(f32), axis=(0, 2))
    partial = jnp.zeros((tok_rows, full_width), bf16)
    for step in range(count):
        partial = lax.dynamic_update_slice_in_dim(
            partial,
            jnp.einsum(
                "mth,mch->tc", grads, w_blocks[step], preferred_element_type=f32
            ).astype(bf16),
            owners[step] * half,
            1,
        )
    grad_normed, norm_dots = reduce_kernel(partial, dots, 2)
    grad_qkv = ring_reduce(
        lambda step: jnp.einsum(
            "tc,mth->mch", columns_of(normed, step), grads, preferred_element_type=f32
        )
    )

    row_gain = jnp.where(picked, norm_gain[1][None, :], norm_gain[0][None, :])
    scaled = layer_input.astype(f32) * inv_rms[:, None]
    upstream = grad_normed * row_gain
    grad_in = (inv_rms[:, None] * (upstream - scaled * (norm_dots / full_width)[:, None])).astype(
        bf16
    )
    weighted = grad_normed * scaled
    local_gain = jnp.stack(
        [
            jnp.sum(jnp.where(modality[:, None] == kind, weighted, 0.0), axis=0)
            for kind in range(norm_gain.shape[0])
        ]
    )
    if count == 2:
        grad_gain = local_gain + shift_ring(local_gain, 1)
    else:
        grad_gain = lax.psum(local_gain, "gz")
    return (attn_out, grad_in, grad_qkv, grad_wout, grad_gain)


def solution(mesh):
    in_specs = (
        P("gz", ("gx", "gy")),
        P("gz"),
        P(),
        P(None, ("gx", "gy")),
        P(None, "gz", ("gx", "gy")),
        P(("gx", "gy"), "gz"),
        P("gz", ("gx", "gy")),
    )
    out_specs = (
        P("gz", ("gx", "gy")),
        P("gz", ("gx", "gy")),
        P(None, "gz", ("gx", "gy")),
        P(("gx", "gy"), "gz"),
        P(None, ("gx", "gy")),
    )
    return jax.shard_map(
        per_device, mesh=mesh, in_specs=in_specs, out_specs=out_specs, check_vma=False
    )
```
